32 devices in a mesh: seq: 8 (over z, x), head: 4 (over y, core).
Axes of the slice: x: 2, y: 2, z: 4, core: 2. Of those that a mesh axis runs over, the one named last changes fastest.
Arguments:
- queries: bfloat16 [8192, 2048], P('seq', 'head'), may hold values from -200 to 200
- keys: bfloat16 [8192, 2048], P('seq', 'head'), may hold values from -6 to 6
- values: bfloat16 [8192, 2048], P('seq', 'head'), may hold values from -12 to 12
- gate_bias: float32 [16], P('head'), may hold values from -2 to 2
- out_weight: bfloat16 [2048, 4096], P(None, 'head'), may hold values from -0.125 to 0.125
Outputs:
- layer_out: bfloat16 [8192, 4096], P('seq', 'head')
The draws below stay inside these ranges and needn't reach their ends.
All inputs are finite; a program needn't handle non-finite values.
Results may differ from the reference program's by a relative error of at most 0.007.
Values may be sent and summed in bfloat16 or wider, within the bound.
A program may use at most 128 MiB of HBM per device.

```python
import jax
import jax.numpy as jnp
from jax import lax

D = 4096
HEADS = 16
DH = 128
SEG = 256
TOKENS = 8192


def sign_field(key, salt, shape):
    flips = jax.random.bernoulli(jax.random.fold_in(key, salt), 0.5, shape)
    return jnp.where(flips, 1.0, -1.0).astype(jnp.float32)


def column_pattern(key):
    per_segment = sign_field(key, 21, (TOKENS // SEG, HEADS * DH))
    return jnp.repeat(per_segment, SEG, axis=0)


def key_signs(key):
    rates = jax.random.uniform(jax.random.fold_in(key, 24), (TOKENS // SEG, HEADS), jnp.float32, 0.2, 0.8)
    coins = jax.random.uniform(jax.random.fold_in(key, 22), (TOKENS, HEADS), jnp.float32)
    signs = jnp.where(coins < jnp.repeat(rates, SEG, axis=0), 1.0, -1.0).astype(jnp.float32)
    return jnp.repeat(signs, DH, axis=1)


def query_signs(key):
    return jnp.repeat(sign_field(key, 23, (TOKENS, HEADS)), DH, axis=1)


def position_shift():
    positions = jnp.arange(TOKENS).astype(jnp.float32)
    return -1.5 + 3.0 * (positions + 0.5) / TOKENS


def key_table(key):
    noise = jax.random.normal(jax.random.fold_in(key, 11), (TOKENS, HEADS * DH), jnp.float32)
    table = noise + 2.0 * key_signs(key) * column_pattern(key) + position_shift()[:, None]
    return jnp.clip(table, -6.0, 6.0)


def draw_keys(key, part):
    return key_table(key).astype(jnp.bfloat16)


def draw_queries(key, part):
    base_draw = jax.random.normal(jax.random.fold_in(key, 12), (TOKENS, HEADS * DH), jnp.float32)
    base_draw = base_draw + 0.75 * query_signs(key) * column_pattern(key)
    return jnp.clip(base_draw, -200.0, 200.0).astype(jnp.bfloat16)


def draw_values(key, part):
    noise = jax.random.normal(jax.random.fold_in(key, 13), (TOKENS, HEADS * DH), jnp.float32)
    column_off = jax.random.normal(jax.random.fold_in(key, 14), (HEADS * DH,), jnp.float32)
    segment_off = jax.random.normal(jax.random.fold_in(key, 15), (TOKENS // SEG, HEADS * DH), jnp.float32)
    linked = jax.random.normal(jax.random.fold_in(key, 16), (TOKENS // SEG, HEADS * DH), jnp.float32)
    table = noise + column_off[None, :] + jnp.repeat(segment_off, SEG, axis=0)
    table = table + 1.5 * key_signs(key) * jnp.repeat(linked, SEG, axis=0)
    return jnp.clip(table, -12.0, 12.0).astype(jnp.bfloat16)


def shard_levels(stream_key, shape, split, least, top_value):
    gain = 1.0
    for dim, parts in split:
        heights = jax.random.uniform(jax.random.fold_in(jax.random.fold_in(stream_key, 6), dim), (parts,), jnp.float32, least / len(split), top_value / len(split))
        gain = gain * jnp.repeat(jnp.exp(heights), shape[dim] // parts).reshape((-1,) + (1,) * (len(shape) - 1 - dim))
    return gain


def scatter_about(own_key, dims, spread, bound, pieces=(), held_as=jnp.bfloat16):
    array = spread * jax.random.normal(own_key, dims, jnp.float32)
    if pieces:
        array = array * shard_levels(own_key, dims, pieces, -0.22, 0.18)
    return jnp.clip(array, -bound, bound).astype(held_as)


def setup_inputs(seed: int = 0) -> dict:
    key_list = jax.random.split(jax.random.key(seed), 6)
    return {
        "queries": draw_queries(jax.random.fold_in(key_list[5], 71), 0),
        "keys": draw_keys(jax.random.fold_in(key_list[5], 71), 0),
        "values": draw_values(jax.random.fold_in(key_list[5], 71), 0),
        "gate_bias": jnp.clip(jax.random.uniform(key_list[3], (HEADS,), jnp.float32, -2.0, 2.0) * shard_levels(key_list[3], (HEADS,), ((0, 4),), -0.4, 0.0), -2.0, 2.0),
        "out_weight": scatter_about(key_list[4], (HEADS * DH, D), (HEADS * DH) ** -0.5, 0.125, ((1, 4),)),
    }


def reference(queries, keys, values, gate_bias, out_weight):
    seg_count = TOKENS // SEG
    blk_shape = (seg_count, SEG, HEADS, DH)
    query_blk = queries.reshape(blk_shape)
    key_blk = keys.reshape(blk_shape)
    value_blk = values.reshape(blk_shape)
    gate_open = jax.nn.sigmoid(gate_bias.astype(jnp.float32))
    positions = jnp.arange(SEG)
    causal = positions[:, None] >= positions[None, :]
    score_scale = 1.0 / (DH ** 0.5)
    high = lax.Precision.HIGHEST

    def segment(state_pair, inputs_seg):
        memory, normalizer = state_pair
        query_seg, key_seg, value_seg = inputs_seg
        query_flt = query_seg.astype(jnp.float32)
        key_flt = key_seg.astype(jnp.float32)
        value_flt = value_seg.astype(jnp.float32)
        query_map = jax.nn.elu(query_flt) + 1.0
        key_map = (jax.nn.elu(key_flt) + 1.0).astype(jnp.bfloat16).astype(jnp.float32)
        recall = jnp.einsum('thd,hde->the', query_map, memory, precision=high)
        denominator = jnp.einsum('thd,hd->th', query_map, normalizer, precision=high) + 1.0
        recall = recall / denominator[:, :, None]
        scores = jnp.einsum('qhd,khd->hqk', query_flt, key_flt, precision=high) * score_scale
        scores = jnp.where(causal[None], scores, jnp.float32(-1e30))
        weights = jax.nn.softmax(scores, axis=-1).astype(jnp.bfloat16).astype(jnp.float32)
        local_out = jnp.einsum('hqk,khd->qhd', weights, value_flt, precision=high)
        mixed = gate_open[None, :, None] * recall + (1.0 - gate_open)[None, :, None] * local_out
        context = mixed.astype(jnp.bfloat16).reshape(SEG, HEADS * DH)
        projected = jnp.dot(context, out_weight, preferred_element_type=jnp.float32).astype(jnp.bfloat16)
        memory = memory + jnp.einsum('thd,the->hde', key_map, value_flt, precision=high)
        normalizer = normalizer + jnp.sum(key_map, axis=0)
        return (memory, normalizer), projected

    start_state = (jnp.zeros((HEADS, DH, DH), jnp.float32), jnp.zeros((HEADS, DH), jnp.float32))
    ignored, outputs = lax.scan(segment, start_state, (query_blk, key_blk, value_blk))
    return outputs.reshape(TOKENS, D)
```

```python
import functools

import jax
import jax.numpy as jnp
from jax import lax
from jax.experimental import pallas as pl
from jax.experimental.pallas import tpu as pltpu
from jax.sharding import PartitionSpec as P

DH = 128
SEG = 256
MEM = DH + 8
PAIR = 2 * DH
MESH = pl.DeviceIdType.MESH
F32 = jnp.float32
BF16 = jnp.bfloat16
NT = (((1,), (1,)), ((), ()))
TN = (((0,), (0,)), ((), ()))


def elu1(x):
    return jnp.where(x > 0.0, x + 1.0, jnp.exp(jnp.minimum(x, 0.0)))


def split(x):
    top = x.astype(BF16)
    return top, (x - top.astype(F32)).astype(BF16)


def kernel(
    ns, nh, q_ref, k_ref, v_ref, gate_ref, w_hbm, out_ref,
    w_ref, local, inner, total, from_pair, from_prev, to_next, prior, ctx, acc,
    w_sem, x_send, x_recv, z_send, z_recv, c_send, c_recv, f_send,
):
    rows, cols = q_ref.shape
    segs, heads = rows // SEG, cols // DH
    pairs = heads // 2
    blocks = segs * heads
    me_s, me_h = lax.axis_index("seq"), lax.axis_index("head")
    z, odd = me_s // 2, lax.rem(me_s, 2)
    zs = ns // 2
    pair_s = me_s + 1 - 2 * odd
    up, down = lax.rem(me_s + 2, ns), lax.rem(me_s + ns - 2, ns)
    group, core = me_h // 2, lax.rem(me_h, 2)
    pair_h = me_h + 1 - 2 * core
    groups = nh // 2

    weight_copy = pltpu.make_async_copy(w_hbm, w_ref, w_sem)
    weight_copy.start()

    barrier = pltpu.get_barrier_semaphore()
    seq_peers = [pair_s, up, down]
    for s in seq_peers:
        pl.semaphore_signal(barrier, inc=1, device_id=(s, me_h), device_id_type=MESH)
    far = [lax.rem(group + d, groups) * 2 + core for d in range(1, groups)]
    for h in [pair_h] + far:
        pl.semaphore_signal(barrier, inc=1, device_id=(me_s, h), device_id_type=MESH)

    def x_copy(h):
        return pltpu.make_async_remote_copy(
            src_ref=total.at[h], dst_ref=from_pair.at[h],
            send_sem=x_send.at[h], recv_sem=x_recv.at[h],
            device_id=(pair_s, me_h), device_id_type=MESH,
        )

    def z_copy(h):
        return pltpu.make_async_remote_copy(
            src_ref=to_next.at[h], dst_ref=from_prev.at[h],
            send_sem=z_send.at[h], recv_sem=z_recv.at[h],
            device_id=(up, me_h), device_id_type=MESH,
        )

    def ctx_copy(source, target, j, s, send):
        part = ctx.at[source * pairs + j, pl.ds(pl.multiple_of(s * SEG, SEG), SEG)]
        return pltpu.make_async_remote_copy(
            src_ref=part, dst_ref=part,
            send_sem=send, recv_sem=c_recv.at[source, j, s],
            device_id=(me_s, target), device_id_type=MESH,
        )

    for h in range(heads):
        span = pl.ds(h * DH, DH)
        run = jnp.zeros((MEM, DH), F32)
        for s in range(segs):
            inner[h, s] = run
            part = pl.ds(s * SEG, SEG)
            key_map = elu1(k_ref[part, span].astype(F32)).astype(BF16)
            delta = lax.dot_general(v_ref[part, span], key_map, TN, preferred_element_type=F32)
            norm = jnp.sum(key_map.astype(F32), axis=0, keepdims=True)
            run = run + jnp.concatenate([delta, jnp.broadcast_to(norm, (8, DH))], axis=0)
        total[h] = run
        if h == 0:
            pl.semaphore_wait(barrier, 3 + 1 + len(far))
        x_copy(h).start()

    @pl.when(z == 0)
    def _():
        from_prev[...] = jnp.zeros_like(from_prev)

    def chain(h):
        x_copy(h).wait_recv()

        @pl.when(z > 0)
        def _():
            z_copy(h).wait_recv()

        before = from_prev[h]
        other = from_pair[h]

        @pl.when(z < zs - 1)
        def _():
            to_next[h] = before + (total[h] + other)
            z_copy(h).start()

        prior[h] = before + jnp.where(odd == 1, other, 0.0)

    row_id = lax.broadcasted_iota(jnp.int32, (SEG, SEG), 0)
    col_id = lax.broadcasted_iota(jnp.int32, (SEG, SEG), 1)
    ones = jnp.ones((SEG, DH), BF16)
    first, hop = 3, 5

    @pl.loop(0, blocks)
    def _(b):
        for c in range(heads):
            @pl.when(b == first + 2 * c + hop * z)
            def _():
                chain(c)
        h, s = b // segs, lax.rem(b, segs)
        span = pl.ds(pl.multiple_of(h * DH, DH), DH)
        part = pl.ds(pl.multiple_of(s * SEG, SEG), SEG)
        scores = lax.dot_general(q_ref[part, span], k_ref[part, span], NT, preferred_element_type=F32)
        scores = jnp.where(row_id >= col_id, scores * (1.0 / DH**0.5), -1e30)
        weights = jnp.exp(scores - jnp.max(scores, axis=1, keepdims=True)).astype(BF16)
        both = jnp.dot(
            weights, jnp.concatenate([v_ref[part, span], ones], axis=1), preferred_element_type=F32
        )
        local[part, span] = both[:, :DH] / both[:, DH:]

    for c in range(heads):
        @pl.when(first + 2 * c + hop * z >= blocks)
        def _():
            chain(c)

    for j in range(pairs):
        gates = [
            1.0 / (1.0 + jnp.exp(-jnp.full((1, DH), gate_ref[2 * j + i], F32))) for i in range(2)
        ]

        @pl.loop(0, segs)
        def _(s):
            part = pl.ds(pl.multiple_of(s * SEG, SEG), SEG)
            mixed = []
            for i in range(2):
                h = 2 * j + i
                span = pl.ds(h * DH, DH)
                mem = prior[h] + inner[h, s]
                mem = jnp.concatenate(
                    [mem[:DH], jnp.broadcast_to(mem[DH : DH + 1], (DH, DH))], axis=0
                )
                m_top, m_low = split(mem)
                q_top, q_low = split(elu1(q_ref[part, span].astype(F32)))
                recall = lax.dot_general(
                    jnp.concatenate([q_top, q_low], axis=1),
                    jnp.concatenate([m_top, m_top], axis=1),
                    NT, preferred_element_type=F32,
                ) + lax.dot_general(q_top, m_low, NT, preferred_element_type=F32)
                recall = recall[:, :DH] / (recall[:, DH:] + 1.0)
                mixed.append(gates[i] * recall + (1.0 - gates[i]) * local[part, span])
            ctx[me_h * pairs + j, part] = jnp.concatenate(mixed, axis=1).astype(BF16)
            for t in far + [pair_h]:
                ctx_copy(me_h, t, j, s, c_send.at[t, j, s]).start()

    weight_copy.wait()

    def product(source, j, part):
        slot = source * pairs + j
        return jnp.dot(
            ctx[slot, part],
            w_ref[pl.ds(pl.multiple_of(slot * PAIR, PAIR), PAIR), :],
            preferred_element_type=F32,
        )

    @pl.loop(0, segs)
    def _(s):
        part = pl.ds(pl.multiple_of(s * SEG, SEG), SEG)
        for j in range(pairs):
            ctx_copy(pair_h, pair_h, j, s, c_send.at[pair_h, j, s]).wait_recv()
        sums = product(me_h, 0, part)
        for j in range(1, pairs):
            sums = sums + product(me_h, j, part)
        for j in range(pairs):
            sums = sums + product(pair_h, j, part)
        acc[part, :] = sums

    for j in range(pairs):
        for f in far:
            twin = (f // 2) * 2 + 1 - core

            @pl.loop(0, segs)
            def _(s):
                part = pl.ds(pl.multiple_of(s * SEG, SEG), SEG)
                ctx_copy(f, pair_h, j, s, c_send.at[f, j, s]).wait_recv()
                ctx_copy(f, pair_h, j, s, f_send.at[f, j, s]).start()
                sums = acc[part, :] + product(f, j, part)
                ctx_copy(twin, pair_h, j, s, c_send.at[f, j, s]).wait_recv()
                acc[part, :] = sums + product(twin, j, part)

    out_ref[...] = acc[...].astype(BF16)

    for h in range(heads):
        x_copy(h).wait_send()

        @pl.when(z < zs - 1)
        def _():
            z_copy(h).wait_send()

    for j in range(pairs):
        @pl.loop(0, segs)
        def _(s):
            for t in far + [pair_h]:
                ctx_copy(me_h, t, j, s, c_send.at[t, j, s]).wait_send()
            for f in far:
                ctx_copy(f, pair_h, j, s, f_send.at[f, j, s]).wait_send()


def body(ns, nh, queries, keys, values, gate_bias, out_weight):
    rows, cols = queries.shape
    depth, outs = out_weight.shape
    segs, heads = rows // SEG, cols // DH
    pairs = heads // 2
    vmem = pl.BlockSpec(memory_space=pltpu.VMEM)
    dma = pltpu.SemaphoreType.DMA
    mem = pltpu.VMEM((heads, MEM, DH), F32)
    return pl.pallas_call(
        functools.partial(kernel, ns, nh),
        out_shape=pltpu.VMEM((rows, outs), BF16),
        in_specs=[vmem, vmem, vmem, pl.BlockSpec(memory_space=pltpu.SMEM),
                  pl.BlockSpec(memory_space=pl.ANY)],
        out_specs=vmem,
        scratch_shapes=[
            pltpu.VMEM((depth, outs), BF16),
            pltpu.VMEM((rows, cols), F32),
            pltpu.VMEM((heads, segs, MEM, DH), F32),
            mem, mem, mem, mem, mem,
            pltpu.VMEM((nh * pairs, rows, PAIR), BF16),
            pltpu.VMEM((rows, outs), F32),
            dma, dma((heads,)), dma((heads,)), dma((heads,)), dma((heads,)),
            dma((nh, pairs, segs)), dma((nh, pairs, segs)), dma((nh, pairs, segs)),
        ],
        compiler_params=pltpu.CompilerParams(
            collective_id=0, has_side_effects=True, vmem_limit_bytes=60 * 1024 * 1024
        ),
        name="infini_layer",
    )(queries, keys, values, gate_bias, out_weight)


def solution(mesh):
    sizes = dict(mesh.shape)
    return jax.shard_map(
        functools.partial(body, sizes["seq"], sizes["head"]),
        mesh=mesh,
        in_specs=(P("seq", "head"), P("seq", "head"), P("seq", "head"), P("head"), P(None, "head")),
        out_specs=P("seq", "head"),
        check_vma=False,
    )
```

```python
import functools

import jax
import jax.numpy as jnp
from jax import lax
from jax.experimental import pallas as pl
from jax.experimental.pallas import tpu as pltpu
from jax.sharding import PartitionSpec as P

DH = 128
SEG = 256
MEM = DH + 8
SENT = DH + 16
X_FIRST = 4
CTX_FIRST = 4
CTX_HOP = 4
MESH = pl.DeviceIdType.MESH
F32 = jnp.float32
BF16 = jnp.bfloat16
NT = (((1,), (1,)), ((), ()))
TN = (((0,), (0,)), ((), ()))


def elu1(x):
    return jnp.where(x > 0.0, x + 1.0, jnp.exp(jnp.minimum(x, 0.0)))


def rows_of(s):
    return pl.ds(pl.multiple_of(s * SEG, SEG), SEG)


def kernel(
    ns, nh, q_hbm, k_hbm, v_hbm, gate_ref, w_hbm, out_ref,
    q_ref, k_ref, v_ref, w_ref, local, inner, total, mine, from_pair, plane, from_plane, prior, ctx, acc,
    in_sem, w_sem, x_send, x_recv, z_send, z_recv, c_send, c_recv, f_send,
):
    heads, rows, _ = q_ref.shape
    segs = rows // SEG
    pairs = heads // 2
    blocks = segs * heads
    me_s, me_h = lax.axis_index("seq"), lax.axis_index("head")
    z, odd = me_s // 2, lax.rem(me_s, 2)
    zs = ns // 2
    pair_s = me_s + 1 - 2 * odd
    group, core = me_h // 2, lax.rem(me_h, 2)
    pair_h = me_h + 1 - 2 * core
    groups = nh // 2

    def load(i, h):
        src, dst = ((k_hbm, k_ref), (v_hbm, v_ref), (q_hbm, q_ref))[i]
        return pltpu.make_async_copy(src.at[:, pl.ds(h * DH, DH)], dst.at[h], in_sem.at[i, h])

    weight_copy = pltpu.make_async_copy(w_hbm, w_ref, w_sem)
    for h in range(heads):
        load(0, h).start()
        load(1, h).start()
    for h in range(heads):
        load(2, h).start()
    weight_copy.start()

    barrier = pltpu.get_barrier_semaphore()
    pl.semaphore_signal(barrier, inc=1, device_id=(pair_s, me_h), device_id_type=MESH)
    for d in range(1, zs):
        peer = lax.rem(z + d, zs) * 2 + odd
        pl.semaphore_signal(barrier, inc=1, device_id=(peer, me_h), device_id_type=MESH)
    far = [lax.rem(group + d, groups) * 2 + core for d in range(1, groups)]
    for h in [pair_h] + far:
        pl.semaphore_signal(barrier, inc=1, device_id=(me_s, h), device_id_type=MESH)

    def x_copy(h):
        return pltpu.make_async_remote_copy(
            src_ref=mine.at[h], dst_ref=from_pair.at[h],
            send_sem=x_send.at[h], recv_sem=x_recv.at[h],
            device_id=(pair_s, me_h), device_id_type=MESH,
        )

    def z_copy(source, target, h):
        return pltpu.make_async_remote_copy(
            src_ref=plane.at[h], dst_ref=from_plane.at[source, h],
            send_sem=z_send.at[target, h], recv_sem=z_recv.at[source, h],
            device_id=(target * 2 + odd, me_h), device_id_type=MESH,
        )

    def ctx_copy(source, target, h, s, send):
        part = ctx.at[source * heads + h, rows_of(s)]
        return pltpu.make_async_remote_copy(
            src_ref=part, dst_ref=part,
            send_sem=send, recv_sem=c_recv.at[source, h, s],
            device_id=(me_s, target), device_id_type=MESH,
        )

    for h in range(heads):
        load(0, h).wait()
        load(1, h).wait()
        run = jnp.zeros((MEM, DH), F32)
        for s in range(segs):
            inner[h, s] = run
            part = pl.ds(s * SEG, SEG)
            key_map = elu1(k_ref[h, part].astype(F32)).astype(BF16)
            delta = lax.dot_general(v_ref[h, part], key_map, TN, preferred_element_type=F32)
            norm = jnp.sum(key_map.astype(F32), axis=0, keepdims=True)
            run = run + jnp.concatenate([delta, jnp.broadcast_to(norm, (8, DH))], axis=0)
        total[h] = run
        mine[h] = jnp.concatenate([run, run[DH:]], axis=0).astype(BF16)
        if h == 0:
            pl.semaphore_wait(barrier, zs + 1 + len(far))
        x_copy(h).start()

    for h in range(heads):
        load(2, h).wait()

    def meet(h):
        x_copy(h).wait_recv()
        other = from_pair[h].astype(F32)[:MEM]
        both = total[h] + other
        plane[h] = jnp.concatenate([both, both[DH:]], axis=0).astype(BF16)

        @pl.loop(0, zs - 1 - z)
        def _(d):
            z_copy(z, zs - 1 - d, h).start()

        prior[h] = jnp.where(odd == 1, other, 0.0)

    def mix(h, s):
        part = rows_of(s)
        gate = 1.0 / (1.0 + jnp.exp(-jnp.full((1, DH), gate_ref[h], F32)))
        mem = prior[h] + inner[h, s]
        mem = jnp.concatenate(
            [mem[:DH], jnp.broadcast_to(mem[DH : DH + 1], (DH, DH))], axis=0
        ).astype(BF16)
        q_map = elu1(q_ref[h, part].astype(F32)).astype(BF16)
        recall = lax.dot_general(q_map, mem, NT, preferred_element_type=F32)
        recall = recall[:, :DH] / (recall[:, DH:] + 1.0)
        ctx[me_h * heads + h, part] = (gate * recall + (1.0 - gate) * local[h, part]).astype(BF16)
        for t in far + [pair_h]:
            ctx_copy(me_h, t, h, s, c_send.at[t, h, s]).start()

    def arrive(h):
        @pl.loop(0, z)
        def _(p):
            z_copy(p, z, h).wait_recv()
            prior[h] = prior[h] + from_plane[p, h].astype(F32)[:MEM]

    def finish(c):
        arrive(c)
        if c < heads - 2:
            @pl.loop(0, segs)
            def _(s):
                mix(c, s)
        elif c == heads - 1:
            @pl.loop(0, segs)
            def _(s):
                mix(c - 1, s)
                mix(c, s)

    row_id = lax.broadcasted_iota(jnp.int32, (SEG, SEG), 0)
    col_id = lax.broadcasted_iota(jnp.int32, (SEG, SEG), 1)
    ones = jnp.ones((SEG, DH), BF16)

    def meet_at(c):
        return X_FIRST + c

    def finish_at(c):
        ready = CTX_FIRST + X_FIRST + CTX_HOP * jnp.minimum(z, 1) + c
        return jnp.maximum(ready, segs * (c + 1))

    @pl.loop(0, blocks)
    def _(b):
        for c in range(heads):
            @pl.when(b == meet_at(c))
            def _():
                meet(c)
        for c in range(heads):
            @pl.when(b == finish_at(c))
            def _():
                finish(c)
        h, s = b // segs, lax.rem(b, segs)
        part = rows_of(s)
        scores = lax.dot_general(q_ref[h, part], k_ref[h, part], NT, preferred_element_type=F32)
        scores = jnp.where(row_id >= col_id, scores * (1.0 / DH**0.5), -1e30)
        weights = jnp.exp(scores - jnp.max(scores, axis=1, keepdims=True)).astype(BF16)
        both = jnp.dot(
            weights, jnp.concatenate([v_ref[h, part], ones], axis=1), preferred_element_type=F32
        )
        local[h, part] = both[:, :DH] / both[:, DH:]

    for c in range(heads):
        if meet_at(c) >= blocks:
            meet(c)
    for c in range(heads):
        @pl.when(finish_at(c) >= blocks)
        def _():
            finish(c)

    weight_copy.wait()

    def product(source, j, part):
        slot = source * heads + 2 * j
        return jnp.dot(
            jnp.concatenate([ctx[slot, part], ctx[slot + 1, part]], axis=1),
            w_ref[pl.ds(pl.multiple_of(slot * DH, 2 * DH), 2 * DH), :],
            preferred_element_type=F32,
        )

    def took(source, h, s):
        ctx_copy(source, pair_h, h, s, c_send.at[pair_h, h, s]).wait_recv()

    def twin_of(f):
        return (f // 2) * 2 + 1 - core

    def relay(f, h, s):
        took(f, h, s)
        ctx_copy(f, pair_h, h, s, f_send.at[f, h, s]).start()

    @pl.loop(0, segs)
    def _(s):
        part = rows_of(s)
        for h in range(heads):
            took(pair_h, h, s)
        sums = product(me_h, 0, part)
        for j in range(1, pairs):
            sums = sums + product(me_h, j, part)
        for j in range(pairs):
            sums = sums + product(pair_h, j, part)
        acc[part, :] = sums

    for j in range(pairs - 1):
        for h in (2 * j, 2 * j + 1):
            for f in far:
                @pl.loop(0, segs)
                def _(s):
                    relay(f, h, s)

        @pl.loop(0, segs)
        def _(s):
            part = rows_of(s)
            sums = acc[part, :]
            for f in far:
                took(twin_of(f), 2 * j, s)
                took(twin_of(f), 2 * j + 1, s)
                sums = sums + product(f, j, part) + product(twin_of(f), j, part)
            acc[part, :] = sums

    last = pairs - 1

    def close(s):
        part = rows_of(s)
        sums = acc[part, :]
        for f in far:
            took(twin_of(f), 2 * last, s)
            took(twin_of(f), 2 * last + 1, s)
            sums = sums + product(twin_of(f), last, part)
        out_ref[part, :] = sums.astype(BF16)

    @pl.loop(0, segs)
    def _(s):
        part = rows_of(s)
        for f in far:
            relay(f, 2 * last, s)
            relay(f, 2 * last + 1, s)
        sums = acc[part, :]
        for f in far:
            sums = sums + product(f, last, part)
        acc[part, :] = sums

        @pl.when(s > 0)
        def _():
            close(s - 1)

    close(segs - 1)

    for h in range(heads):
        x_copy(h).wait_send()

        @pl.loop(z + 1, zs)
        def _(t):
            z_copy(z, t, h).wait_send()

        @pl.loop(0, segs)
        def _(s):
            for t in far + [pair_h]:
                ctx_copy(me_h, t, h, s, c_send.at[t, h, s]).wait_send()
            for f in far:
                ctx_copy(f, pair_h, h, s, f_send.at[f, h, s]).wait_send()


def body(ns, nh, queries, keys, values, gate_bias, out_weight):
    rows, cols = queries.shape
    depth, outs = out_weight.shape
    segs, heads = rows // SEG, cols // DH
    zs = ns // 2
    hbm = pl.BlockSpec(memory_space=pl.ANY)
    dma = pltpu.SemaphoreType.DMA
    held = pltpu.VMEM((heads, rows, DH), BF16)
    mem = pltpu.VMEM((heads, MEM, DH), F32)
    sent = pltpu.VMEM((heads, SENT, DH), BF16)
    return pl.pallas_call(
        functools.partial(kernel, ns, nh),
        out_shape=pltpu.VMEM((rows, outs), BF16),
        in_specs=[hbm, hbm, hbm, pl.BlockSpec(memory_space=pltpu.SMEM), hbm],
        out_specs=pl.BlockSpec(memory_space=pltpu.VMEM),
        scratch_shapes=[
            held, held, held,
            pltpu.VMEM((depth, outs), BF16),
            pltpu.VMEM((heads, rows, DH), F32),
            pltpu.VMEM((heads, segs, MEM, DH), F32),
            mem, sent, sent, sent,
            pltpu.VMEM((zs, heads, SENT, DH), BF16),
            mem,
            pltpu.VMEM((nh * heads, rows, DH), BF16),
            pltpu.VMEM((rows, outs), F32),
            dma((3, heads)), dma, dma((heads,)), dma((heads,)), dma((zs, heads)), dma((zs, heads)),
            dma((nh, heads, segs)), dma((nh, heads, segs)), dma((nh, heads, segs)),
        ],
        compiler_params=pltpu.CompilerParams(
            collective_id=0, has_side_effects=True, vmem_limit_bytes=56 * 1024 * 1024
        ),
        name="infini_layer",
    )(queries, keys, values, gate_bias, out_weight)


def solution(mesh):
    sizes = dict(mesh.shape)
    return jax.shard_map(
        functools.partial(body, sizes["seq"], sizes["head"]),
        mesh=mesh,
        in_specs=(P("seq", "head"), P("seq", "head"), P("seq", "head"), P("head"), P(None, "head")),
        out_specs=P("seq", "head"),
        check_vma=False,
    )
```

```python
import functools

import jax
import jax.numpy as jnp
from jax import lax
from jax.experimental import pallas as pl
from jax.experimental.pallas import tpu as pltpu
from jax.sharding import PartitionSpec as P

DH = 128
SEG = 256
MEM = DH + 8
SENT = DH + 16
EARLY = 2
MEET_FIRST = 4
MEET_GAP = 4
MEET_CORE = 0
MIX_FIRST = 5
MIX_HOP = 3
MESH = pl.DeviceIdType.MESH
F32 = jnp.float32
BF16 = jnp.bfloat16
NT = (((1,), (1,)), ((), ()))
TN = (((0,), (0,)), ((), ()))


def elu1(x):
    return jnp.where(x > 0.0, x + 1.0, jnp.exp(jnp.minimum(x, 0.0)))


def rows_of(s):
    return pl.ds(pl.multiple_of(s * SEG, SEG), SEG)


def cols_of(h):
    return pl.ds(pl.multiple_of(h * DH, DH), DH)


def packed(mem):
    return jnp.concatenate([mem, mem[DH:]], axis=0).astype(BF16)


def recall_of(q, mem):
    mem = jnp.concatenate(
        [mem[:DH], jnp.broadcast_to(mem[DH : DH + 1], (DH, DH))], axis=0
    ).astype(BF16)
    q_map = elu1(q.astype(F32)).astype(BF16)
    both = lax.dot_general(q_map, mem, NT, preferred_element_type=F32)
    return both[:, :DH] / (both[:, DH:] + 1.0)


def kernel(
    ns, nh, q_hbm, k_hbm, v_hbm, gate_hbm, w_hbm, out_ref,
    q_ref, kv_ref, gate_ref, w_ref, local, inner, total, mine, from_pair, plane, from_plane, prior,
    ctx, acc, own_local, own_inner, own_prior, far_early,
    kv_sem, q_sem, gate_sem, w_sem, open_sem, x_send, x_recv, z_send, z_recv,
    pair_send, pair_recv, far_send, far_recv, twin_send, twin_recv, early_send, early_recv, late_recv,
):
    rows, cols = q_ref.shape
    segs, heads = rows // SEG, cols // DH
    pairs = heads // 2
    last = heads - 1
    blocks = segs * heads
    me_s, me_h = lax.axis_index("seq"), lax.axis_index("head")
    z, odd = me_s // 2, lax.rem(me_s, 2)
    zs = ns // 2
    pair_s = me_s + 1 - 2 * odd
    group, core = me_h // 2, lax.rem(me_h, 2)
    pair_h = me_h + 1 - 2 * core
    groups = nh // 2
    far = [lax.rem(group + d, groups) * 2 + core for d in range(1, groups)]
    twin = [lax.rem(group + d, groups) * 2 + 1 - core for d in range(1, groups)]

    def load(i, h):
        src = (k_hbm, v_hbm)[i]
        return pltpu.make_async_copy(src.at[:, cols_of(h)], kv_ref.at[h, i], kv_sem.at[h])

    def loaded(h):
        pltpu.make_async_copy(kv_ref.at[h], kv_ref.at[h], kv_sem.at[h]).wait()

    q_copy = pltpu.make_async_copy(q_hbm, q_ref, q_sem)
    gate_copy = pltpu.make_async_copy(gate_hbm, gate_ref, gate_sem)
    weight_copy = pltpu.make_async_copy(w_hbm, w_ref, w_sem)
    for h in range(heads):
        load(0, h).start()
        load(1, h).start()
    q_copy.start()
    gate_copy.start()
    weight_copy.start()

    barrier = pltpu.get_barrier_semaphore()
    pl.semaphore_signal(barrier, inc=1, device_id=(pair_s, me_h), device_id_type=MESH)
    for h in [pair_h] + far:
        pl.semaphore_signal(barrier, inc=1, device_id=(me_s, h), device_id_type=MESH)

    @pl.loop(z + 1, zs)
    def _(t):
        pl.semaphore_signal(barrier, inc=1, device_id=(t * 2 + odd, me_h), device_id_type=MESH)

    pl.semaphore_wait(barrier, 2 + len(far) + z)

    @pl.loop(0, z)
    def _(p):
        pl.semaphore_signal(open_sem, inc=1, device_id=(p * 2 + odd, me_h), device_id_type=MESH)

    def x_copy(h):
        return pltpu.make_async_remote_copy(
            src_ref=mine.at[h], dst_ref=from_pair.at[h],
            send_sem=x_send, recv_sem=x_recv.at[h],
            device_id=(pair_s, me_h), device_id_type=MESH,
        )

    def z_copy(source, target, h):
        return pltpu.make_async_remote_copy(
            src_ref=plane.at[h], dst_ref=from_plane.at[source, h],
            send_sem=z_send.at[target - source - 1], recv_sem=z_recv.at[source, h],
            device_id=(target * 2 + odd, me_h), device_id_type=MESH,
        )

    def to_head(part, target, send, recv):
        return pltpu.make_async_remote_copy(
            src_ref=part, dst_ref=part, send_sem=send, recv_sem=recv,
            device_id=(me_s, target), device_id_type=MESH,
        )

    def to_pair(part):
        return to_head(part, pair_h, pair_send, pair_recv)

    def to_far(d, part, unit):
        return to_head(part, far[d], far_send.at[d, unit], far_recv.at[groups - 2 - d, unit])

    def from_far(d, part, unit):
        return to_head(part, far[d], far_send.at[d, unit], far_recv.at[d, unit])

    def relay(d, part, unit):
        return to_head(part, pair_h, twin_send.at[d], twin_recv.at[d, unit])

    early_rows = pl.ds(0, EARLY * SEG)
    q_at, local_at, inner_at = 0, EARLY * SEG, 2 * EARLY * SEG
    prior_at = inner_at + (EARLY - 1) * SENT

    def early(d, src, at, recv):
        slot = groups - 2 - d
        return pltpu.make_async_remote_copy(
            src_ref=src, dst_ref=far_early.at[slot, pl.ds(at, src.shape[0])],
            send_sem=early_send.at[d], recv_sem=recv.at[slot],
            device_id=(me_s, far[d]), device_id_type=MESH,
        )

    def early_done(d, at, size, sem):
        part = far_early.at[d, pl.ds(at, size)]
        return to_head(part, far[d], early_send.at[d], sem.at[d])

    def gate_of(h):
        return 1.0 / (1.0 + jnp.exp(-jnp.full((1, DH), gate_ref[h], F32)))

    def gated(mem):
        return packed(jnp.concatenate([gate_of(last) * mem[:DH], mem[DH:]], axis=0))

    for h in range(heads):
        loaded(h)
        run = jnp.zeros((MEM, DH), F32)
        for s in range(segs):
            inner[h, s] = run
            part = pl.ds(s * SEG, SEG)
            key_map = elu1(kv_ref[h, 0, part].astype(F32)).astype(BF16)
            delta = lax.dot_general(kv_ref[h, 1, part], key_map, TN, preferred_element_type=F32)
            norm = jnp.sum(key_map.astype(F32), axis=0, keepdims=True)
            run = run + jnp.concatenate([delta, jnp.broadcast_to(norm, (8, DH))], axis=0)
        total[h] = run
        mine[h] = packed(run)
        x_copy(h).start()
        if h == min(1, last):
            q_copy.wait()
            for d in range(len(far)):
                early(d, q_ref.at[early_rows, cols_of(last)], q_at, early_recv).start()

    gate_copy.wait()
    for s in range(1, EARLY):
        own_inner[pl.ds((s - 1) * SENT, SENT)] = gated(inner[last, s])
    for d in range(len(far)):
        early(d, own_inner, inner_at, early_recv).start()

    def meet(h):
        x_copy(h).wait_recv()
        other = from_pair[h].astype(F32)[:MEM]
        plane[h] = packed(total[h] + other)
        if h == 0:
            @pl.when(z < zs - 1)
            def _():
                pl.semaphore_wait(open_sem, zs - 1 - z)

        @pl.loop(0, zs - 1 - z)
        def _(t):
            z_copy(z, zs - 1 - t, h).start()

        prior[h] = jnp.where(odd == 1, other, 0.0)

    def mix(h, s):
        part = rows_of(s)
        gate = gate_of(h)
        recall = recall_of(q_ref[part, cols_of(h)], prior[h] + inner[h, s])
        ctx[me_h * heads + h, part] = (gate * recall + (1.0 - gate) * local[h, part]).astype(BF16)

    def send_one(h, s, unit):
        part = ctx.at[me_h * heads + h, rows_of(s)]
        for d in range(len(far)):
            to_far(d, part, unit).start()

    def arrive(h):
        @pl.loop(0, z)
        def _(p):
            z_copy(p, z, h).wait_recv()
            prior[h] = prior[h] + from_plane[p, h].astype(F32)[:MEM]

    def both_of(source, s):
        return ctx.at[pl.ds(source * heads + last - 1, 2), rows_of(s)]

    def finish(c):
        arrive(c)
        if c < last - 1:
            @pl.loop(0, segs)
            def _(s):
                mix(c, s)
                send_one(c, s, c)
                to_pair(ctx.at[me_h * heads + c, rows_of(s)]).start()
        elif c == last:
            own_prior[...] = gated(prior[last])
            for d in range(len(far)):
                early(d, own_prior, prior_at, late_recv).start()

            @pl.loop(0, segs)
            def _(s):
                mix(last - 1, s)

                @pl.when(s < EARLY)
                def _():
                    send_one(last - 1, s, last - 1 + s)

                mix(last, s)

                @pl.when(s >= EARLY)
                def _():
                    for d in range(len(far)):
                        to_far(d, both_of(me_h, s), last - 1 + s).start()

                to_pair(both_of(me_h, s)).start()

    row_id = lax.broadcasted_iota(jnp.int32, (SEG, SEG), 0)
    col_id = lax.broadcasted_iota(jnp.int32, (SEG, SEG), 1)
    ones = jnp.ones((SEG, DH), BF16)

    def attend(h, s):
        part = rows_of(s)
        scores = lax.dot_general(
            q_ref[part, cols_of(h)], kv_ref[h, 0, part], NT, preferred_element_type=F32
        )
        scores = jnp.where(row_id >= col_id, scores * (1.0 / DH**0.5), -1e30)
        weights = jnp.exp(scores - jnp.max(scores, axis=1, keepdims=True)).astype(BF16)
        both = jnp.dot(
            weights, jnp.concatenate([kv_ref[h, 1, part], ones], axis=1), preferred_element_type=F32
        )
        local[h, part] = both[:, :DH] / both[:, DH:]

    def send_local():
        own_local[...] = ((1.0 - gate_of(last)) * local[last, early_rows]).astype(BF16)
        for d in range(len(far)):
            early(d, own_local, local_at, early_recv).start()

    def meet_at(c):
        return MEET_FIRST + MEET_CORE * core + MEET_GAP * c

    def finish_at(c):
        done = segs if c == 0 else blocks if c == last else EARLY + segs * (c + 1)
        ready = jnp.maximum(MIX_FIRST + MIX_HOP * jnp.minimum(z, 2) + c, meet_at(c) + 1)
        return jnp.maximum(ready, done)

    @pl.loop(0, blocks)
    def _(b):
        for c in range(heads):
            @pl.when(b == meet_at(c))
            def _():
                meet(c)
        for c in range(heads):
            @pl.when(b == finish_at(c))
            def _():
                finish(c)

        @pl.when(b == segs + EARLY)
        def _():
            send_local()

        first = last * segs
        i = jnp.where(b < segs, b, jnp.where(b < segs + EARLY, b - segs + first, jnp.where(b < first + EARLY, b - EARLY, b)))
        attend(i // segs, lax.rem(i, segs))

    for c in range(heads):
        @pl.when(meet_at(c) >= blocks)
        def _():
            meet(c)
    for c in range(heads):
        @pl.when(finish_at(c) >= blocks)
        def _():
            finish(c)

    weight_copy.wait()

    def product(source, j, part):
        slot = source * heads + 2 * j
        return jnp.dot(
            jnp.concatenate([ctx[slot, part], ctx[slot + 1, part]], axis=1),
            w_ref[pl.ds(pl.multiple_of(slot * DH, 2 * DH), 2 * DH), :],
            preferred_element_type=F32,
        )

    to_pair(ctx.at[pl.ds(pair_h * heads, heads)]).wait_recv()

    @pl.loop(0, segs)
    def _(s):
        part = rows_of(s)
        sums = product(me_h, 0, part)
        for j in range(1, pairs):
            sums = sums + product(me_h, j, part)
        for j in range(pairs):
            sums = sums + product(pair_h, j, part)
        acc[part, :] = sums

    for j in range(pairs - 1):
        for d in range(len(far)):
            for h in (2 * j, 2 * j + 1):
                whole = ctx.at[far[d] * heads + h]
                from_far(d, whole, h).wait_recv()
                relay(d, whole, j).start()
        for d in range(len(far)):
            relay(d, ctx.at[pl.ds(twin[d] * heads + 2 * j, 2)], j).wait_recv()

        @pl.loop(0, segs)
        def _(s):
            part = rows_of(s)
            sums = acc[part, :]
            for d in range(len(far)):
                sums = sums + product(far[d], j, part) + product(twin[d], j, part)
            acc[part, :] = sums

    for d in range(len(far)):
        early_done(d, 0, prior_at, early_recv).wait_recv()
        early_done(d, prior_at, SENT, late_recv).wait_recv()
        for s in range(EARLY):
            mem = far_early[d, pl.ds(prior_at, SENT)].astype(F32)[:MEM]
            if s > 0:
                mem = mem + far_early[d, pl.ds(inner_at + (s - 1) * SENT, SENT)].astype(F32)[:MEM]
            value = recall_of(far_early[d, pl.ds(q_at + s * SEG, SEG)], mem)
            value = value + far_early[d, pl.ds(local_at + s * SEG, SEG)].astype(F32)
            ctx[far[d] * heads + last, pl.ds(s * SEG, SEG)] = value.astype(BF16)

    def close(s):
        part = rows_of(s)
        sums = acc[part, :]
        for d in range(len(far)):
            relay(d, both_of(twin[d], s), pairs - 1 + s).wait_recv()
            sums = sums + product(twin[d], pairs - 1, part)
        out_ref[part, :] = sums.astype(BF16)

    @pl.loop(0, segs)
    def _(s):
        part = rows_of(s)
        for d in range(len(far)):
            @pl.when(s < EARLY)
            def _():
                from_far(d, ctx.at[far[d] * heads + last - 1, part], last - 1 + s).wait_recv()

            @pl.when(s >= EARLY)
            def _():
                from_far(d, both_of(far[d], s), last - 1 + s).wait_recv()

            relay(d, both_of(far[d], s), pairs - 1 + s).start()
        sums = acc[part, :]
        for d in range(len(far)):
            sums = sums + product(far[d], pairs - 1, part)
        acc[part, :] = sums

        @pl.when(s > 0)
        def _():
            close(s - 1)

    pltpu.make_async_remote_copy(
        src_ref=mine, dst_ref=mine, send_sem=x_send, recv_sem=x_recv.at[0],
        device_id=(pair_s, me_h), device_id_type=MESH,
    ).wait_send()

    @pl.loop(z + 1, zs)
    def _(t):
        pltpu.make_async_remote_copy(
            src_ref=plane, dst_ref=plane, send_sem=z_send.at[t - z - 1], recv_sem=z_recv.at[0, 0],
            device_id=(t * 2 + odd, me_h), device_id_type=MESH,
        ).wait_send()

    to_pair(ctx.at[pl.ds(me_h * heads, heads)]).wait_send()
    for d in range(len(far)):
        for h in range(last - 1):
            to_far(d, ctx.at[me_h * heads + h], h).wait_send()
        for s in range(segs):
            part = both_of(me_h, s) if s >= EARLY else ctx.at[me_h * heads + last - 1, rows_of(s)]
            to_far(d, part, last - 1 + s).wait_send()
        early_done(d, 0, prior_at + SENT, early_recv).wait_send()

    close(segs - 1)
    for d in range(len(far)):
        relay(d, ctx.at[pl.ds(far[d] * heads, heads)], 0).wait_send()


def body(ns, nh, queries, keys, values, gate_bias, out_weight):
    rows, cols = queries.shape
    depth, outs = out_weight.shape
    segs, heads = rows // SEG, cols // DH
    pairs = heads // 2
    zs = ns // 2
    fars = nh // 2 - 1
    hbm = pl.BlockSpec(memory_space=pl.ANY)
    dma = pltpu.SemaphoreType.DMA
    mem = pltpu.VMEM((heads, MEM, DH), F32)
    sent = pltpu.VMEM((heads, SENT, DH), BF16)
    return pl.pallas_call(
        functools.partial(kernel, ns, nh),
        out_shape=pltpu.VMEM((rows, outs), BF16),
        in_specs=[hbm, hbm, hbm, hbm, hbm],
        out_specs=pl.BlockSpec(memory_space=pltpu.VMEM),
        scratch_shapes=[
            pltpu.VMEM((rows, cols), BF16),
            pltpu.VMEM((heads, 2, rows, DH), BF16),
            pltpu.SMEM((heads,), F32),
            pltpu.VMEM((depth, outs), BF16),
            pltpu.VMEM((heads, rows, DH), F32),
            pltpu.VMEM((heads, segs, MEM, DH), F32),
            mem, sent, sent, sent,
            pltpu.VMEM((zs - 1, heads, SENT, DH), BF16),
            mem,
            pltpu.VMEM((nh * heads, rows, DH), BF16),
            pltpu.VMEM((rows, outs), F32),
            pltpu.VMEM((EARLY * SEG, DH), BF16),
            pltpu.VMEM(((EARLY - 1) * SENT, DH), BF16),
            pltpu.VMEM((SENT, DH), BF16),
            pltpu.VMEM((fars, 2 * EARLY * SEG + EARLY * SENT, DH), BF16),
            dma((heads,)), dma, dma, dma, pltpu.SemaphoreType.REGULAR,
            dma, dma((heads,)), dma((zs - 1,)), dma((zs - 1, heads)),
            dma, dma, dma((fars, heads - 2 + segs)), dma((fars, heads - 2 + segs)),
            dma((fars,)), dma((fars, pairs - 1 + segs)),
            dma((fars,)), dma((fars,)), dma((fars,)),
        ],
        compiler_params=pltpu.CompilerParams(
            collective_id=0, has_side_effects=True, vmem_limit_bytes=56 * 1024 * 1024
        ),
        name="infini_layer",
    )(queries, keys, values, gate_bias, out_weight)


def solution(mesh):
    sizes = dict(mesh.shape)
    return jax.shard_map(
        functools.partial(body, sizes["seq"], sizes["head"]),
        mesh=mesh,
        in_specs=(P("seq", "head"), P("seq", "head"), P("seq", "head"), P("head"), P(None, "head")),
        out_specs=P("seq", "head"),
        check_vma=False,
    )
```

```python
import functools

import jax
import jax.numpy as jnp
from jax import lax
from jax.experimental import pallas as pl
from jax.experimental.pallas import tpu as pltpu
from jax.sharding import PartitionSpec as P

DH = 128
SEG = 256
MEM = DH + 8
SENT = DH + 16
EARLY = 2
MEET_FIRST = 4
MEET_GAP = 5
MEET_CORE = 0
MIX_FIRST = 5
MIX_HOP = 3
MESH = pl.DeviceIdType.MESH
F32 = jnp.float32
BF16 = jnp.bfloat16
NT = (((1,), (1,)), ((), ()))
TN = (((0,), (0,)), ((), ()))


def elu1(x):
    return jnp.where(x > 0.0, x + 1.0, jnp.exp(jnp.minimum(x, 0.0)))


def rows_of(s):
    return pl.ds(pl.multiple_of(s * SEG, SEG), SEG)


def cols_of(h):
    return pl.ds(pl.multiple_of(h * DH, DH), DH)


def packed(mem):
    return jnp.concatenate([mem, mem[DH:]], axis=0).astype(BF16)


def recall_of(q, mem):
    mem = jnp.concatenate(
        [mem[:DH], jnp.broadcast_to(mem[DH : DH + 1], (DH, DH))], axis=0
    ).astype(BF16)
    q_map = elu1(q.astype(F32)).astype(BF16)
    both = lax.dot_general(q_map, mem, NT, preferred_element_type=F32)
    return both[:, :DH] / (both[:, DH:] + 1.0)


def kernel(
    ns, nh, q_hbm, k_hbm, v_hbm, gate_hbm, w_hbm, out_ref,
    q_ref, kv_ref, gate_ref, w_ref, local, inner, total, mine, from_pair, plane, from_plane, prior,
    ctx, acc, own_local, own_inner, own_prior, far_early,
    kv_sem, q_sem, gate_sem, w_sem, open_sem, x_send, x_recv, z_send, z_recv,
    pair_send, pair_recv, far_send, far_recv, twin_send, twin_recv, early_send, early_recv, late_recv,
):
    rows, cols = q_ref.shape
    segs, heads = rows // SEG, cols // DH
    pairs = heads // 2
    last = heads - 1
    blocks = segs * heads
    me_s, me_h = lax.axis_index("seq"), lax.axis_index("head")
    z, odd = me_s // 2, lax.rem(me_s, 2)
    zs = ns // 2
    pair_s = me_s + 1 - 2 * odd
    group, core = me_h // 2, lax.rem(me_h, 2)
    pair_h = me_h + 1 - 2 * core
    groups = nh // 2
    ahead = z > 0
    far = [lax.rem(group + d, groups) * 2 + core for d in range(1, groups)]
    twin = [lax.rem(group + d, groups) * 2 + 1 - core for d in range(1, groups)]

    def load(i, h):
        src = (k_hbm, v_hbm)[i]
        return pltpu.make_async_copy(src.at[:, cols_of(h)], kv_ref.at[h, i], kv_sem.at[h])

    def loaded(h):
        pltpu.make_async_copy(kv_ref.at[h], kv_ref.at[h], kv_sem.at[h]).wait()

    q_copy = pltpu.make_async_copy(q_hbm, q_ref, q_sem)
    gate_copy = pltpu.make_async_copy(gate_hbm, gate_ref, gate_sem)
    weight_copy = pltpu.make_async_copy(w_hbm, w_ref, w_sem)
    for h in range(heads):
        load(0, h).start()
        load(1, h).start()
    q_copy.start()
    gate_copy.start()
    weight_copy.start()

    barrier = pltpu.get_barrier_semaphore()
    pl.semaphore_signal(barrier, inc=1, device_id=(pair_s, me_h), device_id_type=MESH)
    for h in [pair_h] + far:
        pl.semaphore_signal(barrier, inc=1, device_id=(me_s, h), device_id_type=MESH)

    @pl.loop(z + 1, zs)
    def _(t):
        pl.semaphore_signal(barrier, inc=1, device_id=(t * 2 + odd, me_h), device_id_type=MESH)

    pl.semaphore_wait(barrier, 2 + len(far) + z)

    @pl.loop(0, z)
    def _(p):
        pl.semaphore_signal(open_sem, inc=1, device_id=(p * 2 + odd, me_h), device_id_type=MESH)

    def x_copy(h):
        return pltpu.make_async_remote_copy(
            src_ref=mine.at[h], dst_ref=from_pair.at[h],
            send_sem=x_send, recv_sem=x_recv.at[h],
            device_id=(pair_s, me_h), device_id_type=MESH,
        )

    def z_copy(source, target, h):
        return pltpu.make_async_remote_copy(
            src_ref=plane.at[h], dst_ref=from_plane.at[source, h],
            send_sem=z_send.at[target - source - 1], recv_sem=z_recv.at[source, h],
            device_id=(target * 2 + odd, me_h), device_id_type=MESH,
        )

    def to_head(part, target, send, recv):
        return pltpu.make_async_remote_copy(
            src_ref=part, dst_ref=part, send_sem=send, recv_sem=recv,
            device_id=(me_s, target), device_id_type=MESH,
        )

    def to_pair(part, j):
        return to_head(part, pair_h, pair_send, pair_recv.at[j])

    def to_far(d, part, unit):
        return to_head(part, far[d], far_send.at[d, unit], far_recv.at[groups - 2 - d, unit])

    def from_far(d, part, unit):
        return to_head(part, far[d], far_send.at[d, unit], far_recv.at[d, unit])

    def relay(d, part, unit):
        return to_head(part, pair_h, twin_send.at[d], twin_recv.at[d, unit])

    early_rows = pl.ds(0, EARLY * SEG)
    q_at, local_at, inner_at = 0, EARLY * SEG, 2 * EARLY * SEG
    prior_at = inner_at + (EARLY - 1) * SENT

    def early(d, src, at, recv):
        slot = groups - 2 - d
        return pltpu.make_async_remote_copy(
            src_ref=src, dst_ref=far_early.at[slot, pl.ds(at, src.shape[0])],
            send_sem=early_send.at[d], recv_sem=recv.at[slot],
            device_id=(me_s, far[d]), device_id_type=MESH,
        )

    def early_done(d, at, size, sem):
        part = far_early.at[d, pl.ds(at, size)]
        return to_head(part, far[d], early_send.at[d], sem.at[d])

    def gate_of(h):
        return 1.0 / (1.0 + jnp.exp(-jnp.full((1, DH), gate_ref[h], F32)))

    def gated(mem):
        return packed(jnp.concatenate([gate_of(last) * mem[:DH], mem[DH:]], axis=0))

    for h in range(heads):
        loaded(h)
        run = jnp.zeros((MEM, DH), F32)
        for s in range(segs):
            inner[h, s] = run
            part = pl.ds(s * SEG, SEG)
            key_map = elu1(kv_ref[h, 0, part].astype(F32)).astype(BF16)
            delta = lax.dot_general(kv_ref[h, 1, part], key_map, TN, preferred_element_type=F32)
            norm = jnp.sum(key_map.astype(F32), axis=0, keepdims=True)
            run = run + jnp.concatenate([delta, jnp.broadcast_to(norm, (8, DH))], axis=0)
        total[h] = run
        mine[h] = packed(run)
        x_copy(h).start()
        if h == min(1, last):
            q_copy.wait()

            @pl.when(ahead)
            def _():
                for d in range(len(far)):
                    early(d, q_ref.at[early_rows, cols_of(last)], q_at, early_recv).start()

    gate_copy.wait()

    @pl.when(ahead)
    def _():
        for s in range(1, EARLY):
            own_inner[pl.ds((s - 1) * SENT, SENT)] = gated(inner[last, s])
        for d in range(len(far)):
            early(d, own_inner, inner_at, early_recv).start()

    def meet(h):
        x_copy(h).wait_recv()
        other = from_pair[h].astype(F32)[:MEM]
        plane[h] = packed(total[h] + other)
        if h == 0:
            @pl.when(z < zs - 1)
            def _():
                pl.semaphore_wait(open_sem, zs - 1 - z)

        @pl.loop(0, zs - 1 - z)
        def _(t):
            z_copy(z, jnp.where(z == 0, zs - 1 - t, z + 1 + t), h).start()

        prior[h] = jnp.where(odd == 1, other, 0.0)

    def mix(h, s):
        part = rows_of(s)
        gate = gate_of(h)
        recall = recall_of(q_ref[part, cols_of(h)], prior[h] + inner[h, s])
        ctx[me_h * heads + h, part] = (gate * recall + (1.0 - gate) * local[h, part]).astype(BF16)

    def send_one(h, s, unit):
        part = ctx.at[me_h * heads + h, rows_of(s)]
        for d in range(len(far)):
            to_far(d, part, unit).start()

    def arrive(h):
        @pl.loop(0, z)
        def _(p):
            z_copy(p, z, h).wait_recv()
            prior[h] = prior[h] + from_plane[p, h].astype(F32)[:MEM]

    def both_of(source, s):
        return ctx.at[pl.ds(source * heads + last - 1, 2), rows_of(s)]

    def finish(c):
        arrive(c)
        if c < last - 1:
            @pl.loop(0, segs)
            def _(s):
                mix(c, s)
                send_one(c, s, c)
                to_pair(ctx.at[me_h * heads + c, rows_of(s)], c // 2).start()
        elif c == last:
            @pl.when(ahead)
            def _():
                own_prior[...] = gated(prior[last])
                for d in range(len(far)):
                    early(d, own_prior, prior_at, late_recv).start()

            @pl.loop(0, segs)
            def _(s):
                mix(last - 1, s)

                alone = jnp.logical_and(ahead, s < EARLY)

                @pl.when(alone)
                def _():
                    send_one(last - 1, s, last - 1 + s)

                mix(last, s)

                @pl.when(jnp.logical_not(alone))
                def _():
                    for d in range(len(far)):
                        to_far(d, both_of(me_h, s), last - 1 + s).start()

                to_pair(both_of(me_h, s), pairs - 1).start()

    row_id = lax.broadcasted_iota(jnp.int32, (SEG, SEG), 0)
    col_id = lax.broadcasted_iota(jnp.int32, (SEG, SEG), 1)
    ones = jnp.ones((SEG, DH), BF16)

    def attend(h, s):
        part = rows_of(s)
        scores = lax.dot_general(
            q_ref[part, cols_of(h)], kv_ref[h, 0, part], NT, preferred_element_type=F32
        )
        scores = jnp.where(row_id >= col_id, scores * (1.0 / DH**0.5), -1e30)
        weights = jnp.exp(scores - jnp.max(scores, axis=1, keepdims=True)).astype(BF16)
        both = jnp.dot(
            weights, jnp.concatenate([kv_ref[h, 1, part], ones], axis=1), preferred_element_type=F32
        )
        local[h, part] = both[:, :DH] / both[:, DH:]

    def send_local():
        own_local[...] = ((1.0 - gate_of(last)) * local[last, early_rows]).astype(BF16)
        for d in range(len(far)):
            early(d, own_local, local_at, early_recv).start()

    def meet_at(c):
        return MEET_FIRST + MEET_CORE * core + MEET_GAP * c

    def finish_at(c):
        done = segs if c == 0 else blocks if c == last else EARLY + segs * (c + 1)
        ready = jnp.maximum(MIX_FIRST + MIX_HOP * jnp.minimum(z, 2) + c, meet_at(c) + 1)
        ready = jnp.maximum(ready, done)
        return ready if c == 0 else jnp.where(ahead, blocks, ready)

    @pl.loop(0, blocks)
    def _(b):
        for c in range(heads):
            @pl.when(b == meet_at(c))
            def _():
                meet(c)
        for c in range(last - 1):
            @pl.when(b == finish_at(c))
            def _():
                finish(c)

        @pl.when(jnp.logical_and(ahead, b == segs + EARLY))
        def _():
            send_local()

        first = last * segs
        i = jnp.where(b < segs, b, jnp.where(b < segs + EARLY, b - segs + first, jnp.where(b < first + EARLY, b - EARLY, b)))
        attend(i // segs, lax.rem(i, segs))

    for c in range(heads):
        @pl.when(meet_at(c) >= blocks)
        def _():
            meet(c)
    for c in range(last - 1):
        @pl.when(finish_at(c) >= blocks)
        def _():
            finish(c)

    weight_copy.wait()

    def product(source, j, part):
        slot = source * heads + 2 * j
        return jnp.dot(
            jnp.concatenate([ctx[slot, part], ctx[slot + 1, part]], axis=1),
            w_ref[pl.ds(pl.multiple_of(slot * DH, 2 * DH), 2 * DH), :],
            preferred_element_type=F32,
        )

    def pair_of(source, j):
        return ctx.at[pl.ds(source * heads + 2 * j, 2)]

    for j in range(pairs - 1):
        to_pair(pair_of(pair_h, j), j).wait_recv()
        for s in range(segs):
            part = rows_of(s)
            sums = product(me_h, j, part) + product(pair_h, j, part)
            acc[part, :] = sums if j == 0 else acc[part, :] + sums

    finish(last - 1)
    finish(last)

    for j in range(pairs - 1):
        for d in range(len(far)):
            for h in (2 * j, 2 * j + 1):
                whole = ctx.at[far[d] * heads + h]
                from_far(d, whole, h).wait_recv()
                relay(d, whole, j).start()

    def cross(d):
        early_done(d, 0, prior_at, early_recv).wait_recv()
        early_done(d, prior_at, SENT, late_recv).wait_recv()
        for s in range(EARLY):
            mem = far_early[d, pl.ds(prior_at, SENT)].astype(F32)[:MEM]
            if s > 0:
                mem = mem + far_early[d, pl.ds(inner_at + (s - 1) * SENT, SENT)].astype(F32)[:MEM]
            value = recall_of(far_early[d, pl.ds(q_at + s * SEG, SEG)], mem)
            value = value + far_early[d, pl.ds(local_at + s * SEG, SEG)].astype(F32)
            ctx[far[d] * heads + last, pl.ds(s * SEG, SEG)] = value.astype(BF16)

    def take(s):
        for d in range(len(far)):
            two = both_of(far[d], s)
            if s < EARLY:
                @pl.when(ahead)
                def _():
                    one = ctx.at[far[d] * heads + last - 1, rows_of(s)]
                    from_far(d, one, last - 1 + s).wait_recv()

                @pl.when(jnp.logical_not(ahead))
                def _():
                    from_far(d, two, last - 1 + s).wait_recv()
            else:
                from_far(d, two, last - 1 + s).wait_recv()
            relay(d, two, pairs - 1 + s).start()

    def twins(s):
        for d in range(len(far)):
            relay(d, both_of(twin[d], s), pairs - 1 + s).wait_recv()

    def tail(sources, s):
        sums = acc[rows_of(s), :]
        for source in sources:
            sums = sums + product(source, pairs - 1, rows_of(s))
        return sums

    def fill(s):
        part = rows_of(s)
        sums = product(me_h, pairs - 1, part) + product(pair_h, pairs - 1, part)
        for j in range(pairs - 1):
            for d in range(len(far)):
                sums = sums + product(far[d], j, part) + product(twin[d], j, part)
        acc[part, :] = acc[part, :] + sums if pairs > 1 else sums

    to_pair(pair_of(pair_h, pairs - 1), pairs - 1).wait_recv()
    for j in range(pairs - 1):
        for d in range(len(far)):
            relay(d, pair_of(twin[d], j), j).wait_recv()
    for s in range(segs):
        if s == min(1, segs - 1):
            @pl.when(ahead)
            def _():
                for d in range(len(far)):
                    cross(d)
        if 0 < s <= EARLY:
            take(s - 1)
        fill(s)
    for s in range(EARLY):
        twins(s)
        out_ref[rows_of(s), :] = tail(far + twin, s).astype(BF16)
    for s in range(EARLY, segs - 1):
        take(s)
        twins(s)
        out_ref[rows_of(s), :] = tail(far + twin, s).astype(BF16)
    take(segs - 1)
    acc[rows_of(segs - 1), :] = tail(far, segs - 1)

    pltpu.make_async_remote_copy(
        src_ref=mine, dst_ref=mine, send_sem=x_send, recv_sem=x_recv.at[0],
        device_id=(pair_s, me_h), device_id_type=MESH,
    ).wait_send()

    @pl.loop(z + 1, zs)
    def _(t):
        pltpu.make_async_remote_copy(
            src_ref=plane, dst_ref=plane, send_sem=z_send.at[t - z - 1], recv_sem=z_recv.at[0, 0],
            device_id=(t * 2 + odd, me_h), device_id_type=MESH,
        ).wait_send()

    to_pair(ctx.at[pl.ds(me_h * heads, heads)], 0).wait_send()
    for d in range(len(far)):
        for h in range(last - 1):
            to_far(d, ctx.at[me_h * heads + h], h).wait_send()
        for s in range(EARLY, segs):
            to_far(d, both_of(me_h, s), last - 1 + s).wait_send()

        @pl.when(ahead)
        def _():
            for s in range(EARLY):
                one = ctx.at[me_h * heads + last - 1, rows_of(s)]
                to_far(d, one, last - 1 + s).wait_send()
            early_done(d, 0, prior_at + SENT, early_recv).wait_send()

        @pl.when(jnp.logical_not(ahead))
        def _():
            for s in range(EARLY):
                to_far(d, both_of(me_h, s), last - 1 + s).wait_send()

    twins(segs - 1)
    out_ref[rows_of(segs - 1), :] = tail(twin, segs - 1).astype(BF16)
    for d in range(len(far)):
        relay(d, ctx.at[pl.ds(far[d] * heads, heads)], 0).wait_send()


def body(ns, nh, queries, keys, values, gate_bias, out_weight):
    rows, cols = queries.shape
    depth, outs = out_weight.shape
    segs, heads = rows // SEG, cols // DH
    pairs = heads // 2
    zs = ns // 2
    fars = nh // 2 - 1
    hbm = pl.BlockSpec(memory_space=pl.ANY)
    dma = pltpu.SemaphoreType.DMA
    mem = pltpu.VMEM((heads, MEM, DH), F32)
    sent = pltpu.VMEM((heads, SENT, DH), BF16)
    return pl.pallas_call(
        functools.partial(kernel, ns, nh),
        out_shape=pltpu.VMEM((rows, outs), BF16),
        in_specs=[hbm, hbm, hbm, hbm, hbm],
        out_specs=pl.BlockSpec(memory_space=pltpu.VMEM),
        scratch_shapes=[
            pltpu.VMEM((rows, cols), BF16),
            pltpu.VMEM((heads, 2, rows, DH), BF16),
            pltpu.SMEM((heads,), F32),
            pltpu.VMEM((depth, outs), BF16),
            pltpu.VMEM((heads, rows, DH), F32),
            pltpu.VMEM((heads, segs, MEM, DH), F32),
            mem, sent, sent, sent,
            pltpu.VMEM((zs - 1, heads, SENT, DH), BF16),
            mem,
            pltpu.VMEM((nh * heads, rows, DH), BF16),
            pltpu.VMEM((rows, outs), F32),
            pltpu.VMEM((EARLY * SEG, DH), BF16),
            pltpu.VMEM(((EARLY - 1) * SENT, DH), BF16),
            pltpu.VMEM((SENT, DH), BF16),
            pltpu.VMEM((fars, 2 * EARLY * SEG + EARLY * SENT, DH), BF16),
            dma((heads,)), dma, dma, dma, pltpu.SemaphoreType.REGULAR,
            dma, dma((heads,)), dma((zs - 1,)), dma((zs - 1, heads)),
            dma, dma((pairs,)), dma((fars, heads - 2 + segs)), dma((fars, heads - 2 + segs)),
            dma((fars,)), dma((fars, pairs - 1 + segs)),
            dma((fars,)), dma((fars,)), dma((fars,)),
        ],
        compiler_params=pltpu.CompilerParams(
            collective_id=0, has_side_effects=True, vmem_limit_bytes=56 * 1024 * 1024
        ),
        name="infini_layer",
    )(queries, keys, values, gate_bias, out_weight)


def solution(mesh):
    sizes = dict(mesh.shape)
    return jax.shard_map(
        functools.partial(body, sizes["seq"], sizes["head"]),
        mesh=mesh,
        in_specs=(P("seq", "head"), P("seq", "head"), P("seq", "head"), P("head"), P(None, "head")),
        out_specs=P("seq", "head"),
        check_vma=False,
    )
```

```python
import functools

import jax
import jax.numpy as jnp
from jax import lax
from jax.experimental import pallas as pl
from jax.experimental.pallas import tpu as pltpu
from jax.sharding import PartitionSpec as P

DH = 128
SEG = 256
MEM = DH + 8
SENT = DH + 16
EARLY = 2
MEET_FIRST = 4
MEET_GAP = 5
MEET_CORE = 0
MIX_FIRST = 5
MIX_HOP = 3
MESH = pl.DeviceIdType.MESH
F32 = jnp.float32
BF16 = jnp.bfloat16
NT = (((1,), (1,)), ((), ()))
TN = (((0,), (0,)), ((), ()))


def elu1(x):
    return jnp.where(x > 0.0, x + 1.0, jnp.exp(jnp.minimum(x, 0.0)))


def rows_of(s):
    return pl.ds(pl.multiple_of(s * SEG, SEG), SEG)


def cols_of(h):
    return pl.ds(pl.multiple_of(h * DH, DH), DH)


def packed(mem):
    return jnp.concatenate([mem, mem[DH:]], axis=0).astype(BF16)


def recall_of(q, mem):
    mem = jnp.concatenate(
        [mem[:DH], jnp.broadcast_to(mem[DH : DH + 1], (DH, DH))], axis=0
    ).astype(BF16)
    q_map = elu1(q.astype(F32)).astype(BF16)
    both = lax.dot_general(q_map, mem, NT, preferred_element_type=F32)
    return both[:, :DH] / (both[:, DH:] + 1.0)


def kernel(
    ns, nh, q_hbm, k_hbm, v_hbm, gate_hbm, w_hbm, out_ref,
    q_ref, kv_ref, gate_ref, w_ref, local, inner, total, mine, from_pair, plane, from_plane, prior,
    ctx, acc, own_local, own_inner, own_prior, far_early,
    kv_sem, q_sem, gate_sem, w_sem, open_sem, x_send, x_recv, z_send, z_recv,
    pair_send, pair_recv, far_send, far_recv, twin_send, twin_recv, early_send, early_recv, late_recv,
):
    rows, cols = q_ref.shape
    segs, heads = rows // SEG, cols // DH
    pairs = heads // 2
    last = heads - 1
    blocks = segs * heads
    me_s, me_h = lax.axis_index("seq"), lax.axis_index("head")
    z, odd = me_s // 2, lax.rem(me_s, 2)
    zs = ns // 2
    pair_s = me_s + 1 - 2 * odd
    group, core = me_h // 2, lax.rem(me_h, 2)
    pair_h = me_h + 1 - 2 * core
    groups = nh // 2
    ahead = z > 0
    far = [lax.rem(group + d, groups) * 2 + core for d in range(1, groups)]
    twin = [lax.rem(group + d, groups) * 2 + 1 - core for d in range(1, groups)]

    def load(i, h):
        src = (k_hbm, v_hbm)[i]
        return pltpu.make_async_copy(src.at[:, cols_of(h)], kv_ref.at[h, i], kv_sem.at[h])

    def loaded(h):
        pltpu.make_async_copy(kv_ref.at[h], kv_ref.at[h], kv_sem.at[h]).wait()

    q_copy = pltpu.make_async_copy(q_hbm, q_ref, q_sem)
    gate_copy = pltpu.make_async_copy(gate_hbm, gate_ref, gate_sem)
    weight_copy = pltpu.make_async_copy(w_hbm, w_ref, w_sem)
    for h in range(heads):
        load(0, h).start()
        load(1, h).start()
    q_copy.start()
    gate_copy.start()

    barrier = pltpu.get_barrier_semaphore()
    pl.semaphore_signal(barrier, inc=1, device_id=(pair_s, me_h), device_id_type=MESH)
    for h in [pair_h] + far:
        pl.semaphore_signal(barrier, inc=1, device_id=(me_s, h), device_id_type=MESH)

    @pl.loop(z + 1, zs)
    def _(t):
        pl.semaphore_signal(barrier, inc=1, device_id=(t * 2 + odd, me_h), device_id_type=MESH)

    pl.semaphore_wait(barrier, 2 + len(far) + z)

    @pl.loop(0, z)
    def _(p):
        pl.semaphore_signal(open_sem, inc=1, device_id=(p * 2 + odd, me_h), device_id_type=MESH)

    def x_copy(h):
        return pltpu.make_async_remote_copy(
            src_ref=mine.at[h], dst_ref=from_pair.at[h],
            send_sem=x_send, recv_sem=x_recv.at[h],
            device_id=(pair_s, me_h), device_id_type=MESH,
        )

    def z_copy(source, target, h):
        return pltpu.make_async_remote_copy(
            src_ref=plane.at[h], dst_ref=from_plane.at[source, h],
            send_sem=z_send.at[target - source - 1], recv_sem=z_recv.at[source, h],
            device_id=(target * 2 + odd, me_h), device_id_type=MESH,
        )

    def to_head(part, target, send, recv):
        return pltpu.make_async_remote_copy(
            src_ref=part, dst_ref=part, send_sem=send, recv_sem=recv,
            device_id=(me_s, target), device_id_type=MESH,
        )

    def to_pair(part, j):
        return to_head(part, pair_h, pair_send, pair_recv.at[j])

    def to_far(d, part, unit):
        return to_head(part, far[d], far_send.at[d, unit], far_recv.at[groups - 2 - d, unit])

    def from_far(d, part, unit):
        return to_head(part, far[d], far_send.at[d, unit], far_recv.at[d, unit])

    def relay(d, part, unit):
        return to_head(part, pair_h, twin_send.at[d], twin_recv.at[d, unit])

    early_rows = pl.ds(0, EARLY * SEG)
    q_at, local_at, inner_at = 0, EARLY * SEG, 2 * EARLY * SEG
    prior_at = inner_at + (EARLY - 1) * SENT

    def early(d, src, at, recv):
        slot = groups - 2 - d
        return pltpu.make_async_remote_copy(
            src_ref=src, dst_ref=far_early.at[slot, pl.ds(at, src.shape[0])],
            send_sem=early_send.at[d], recv_sem=recv.at[slot],
            device_id=(me_s, far[d]), device_id_type=MESH,
        )

    def early_done(d, at, size, sem):
        part = far_early.at[d, pl.ds(at, size)]
        return to_head(part, far[d], early_send.at[d], sem.at[d])

    def gate_of(h):
        return 1.0 / (1.0 + jnp.exp(-jnp.full((1, DH), gate_ref[h], F32)))

    def gated(mem):
        return packed(jnp.concatenate([gate_of(last) * mem[:DH], mem[DH:]], axis=0))

    for h in range(heads):
        loaded(h)
        run = jnp.zeros((MEM, DH), F32)
        for s in range(segs):
            inner[h, s] = run
            part = pl.ds(s * SEG, SEG)
            key_map = elu1(kv_ref[h, 0, part].astype(F32)).astype(BF16)
            delta = lax.dot_general(kv_ref[h, 1, part], key_map, TN, preferred_element_type=F32)
            norm = jnp.sum(key_map.astype(F32), axis=0, keepdims=True)
            run = run + jnp.concatenate([delta, jnp.broadcast_to(norm, (8, DH))], axis=0)
        total[h] = run
        mine[h] = packed(run)
        x_copy(h).start()
        if h == min(1, last):
            q_copy.wait()

            @pl.when(ahead)
            def _():
                for d in range(len(far)):
                    early(d, q_ref.at[early_rows, cols_of(last)], q_at, early_recv).start()

    weight_copy.start()
    gate_copy.wait()

    @pl.when(ahead)
    def _():
        for s in range(1, EARLY):
            own_inner[pl.ds((s - 1) * SENT, SENT)] = gated(inner[last, s])
        for d in range(len(far)):
            early(d, own_inner, inner_at, early_recv).start()

    def meet(h):
        x_copy(h).wait_recv()
        other = from_pair[h].astype(F32)[:MEM]
        plane[h] = packed(total[h] + other)
        if h == 0:
            @pl.when(z < zs - 1)
            def _():
                pl.semaphore_wait(open_sem, zs - 1 - z)

        @pl.loop(0, zs - 1 - z)
        def _(t):
            z_copy(z, jnp.where(z == 0, zs - 1 - t, z + 1 + t), h).start()

        prior[h] = jnp.where(odd == 1, other, 0.0)

    def mix(h, s):
        part = rows_of(s)
        gate = gate_of(h)
        recall = recall_of(q_ref[part, cols_of(h)], prior[h] + inner[h, s])
        ctx[me_h * heads + h, part] = (gate * recall + (1.0 - gate) * local[h, part]).astype(BF16)

    def send_one(h, s, unit):
        part = ctx.at[me_h * heads + h, rows_of(s)]
        for d in range(len(far)):
            to_far(d, part, unit).start()

    def arrive(h):
        @pl.loop(0, z)
        def _(p):
            z_copy(p, z, h).wait_recv()
            prior[h] = prior[h] + from_plane[p, h].astype(F32)[:MEM]

    def both_of(source, s):
        return ctx.at[pl.ds(source * heads + last - 1, 2), rows_of(s)]

    def finish(c):
        arrive(c)
        if c < last - 1:
            @pl.loop(0, segs)
            def _(s):
                mix(c, s)
                send_one(c, s, c)
                to_pair(ctx.at[me_h * heads + c, rows_of(s)], c // 2).start()
        elif c == last:
            @pl.when(ahead)
            def _():
                own_prior[...] = gated(prior[last])
                for d in range(len(far)):
                    early(d, own_prior, prior_at, late_recv).start()

            @pl.loop(0, segs)
            def _(s):
                mix(last - 1, s)

                alone = jnp.logical_and(ahead, s < EARLY)

                @pl.when(alone)
                def _():
                    send_one(last - 1, s, last - 1 + s)

                mix(last, s)

                @pl.when(jnp.logical_not(alone))
                def _():
                    for d in range(len(far)):
                        to_far(d, both_of(me_h, s), last - 1 + s).start()

                to_pair(both_of(me_h, s), pairs - 1).start()

    row_id = lax.broadcasted_iota(jnp.int32, (SEG, SEG), 0)
    col_id = lax.broadcasted_iota(jnp.int32, (SEG, SEG), 1)
    ones = jnp.ones((SEG, DH), BF16)

    def attend(h, s):
        part = rows_of(s)
        scores = lax.dot_general(
            q_ref[part, cols_of(h)], kv_ref[h, 0, part], NT, preferred_element_type=F32
        )
        scores = jnp.where(row_id >= col_id, scores * (1.0 / DH**0.5), -1e30)
        weights = jnp.exp(scores - jnp.max(scores, axis=1, keepdims=True)).astype(BF16)
        both = jnp.dot(
            weights, jnp.concatenate([kv_ref[h, 1, part], ones], axis=1), preferred_element_type=F32
        )
        local[h, part] = both[:, :DH] / both[:, DH:]

    def send_local():
        own_local[...] = ((1.0 - gate_of(last)) * local[last, early_rows]).astype(BF16)
        for d in range(len(far)):
            early(d, own_local, local_at, early_recv).start()

    def meet_at(c):
        return MEET_FIRST + MEET_CORE * core + MEET_GAP * c

    def finish_at(c):
        done = segs if c == 0 else blocks if c == last else EARLY + segs * (c + 1)
        ready = jnp.maximum(MIX_FIRST + MIX_HOP * jnp.minimum(z, 2) + c, meet_at(c) + 1)
        ready = jnp.maximum(ready, done)
        return ready if c == 0 else jnp.where(ahead, blocks, ready)

    @pl.loop(0, blocks)
    def _(b):
        for c in range(heads):
            @pl.when(b == meet_at(c))
            def _():
                meet(c)
        for c in range(last - 1):
            @pl.when(b == finish_at(c))
            def _():
                finish(c)

        @pl.when(jnp.logical_and(ahead, b == segs + EARLY))
        def _():
            send_local()

        first = last * segs
        i = jnp.where(b < segs, b, jnp.where(b < segs + EARLY, b - segs + first, jnp.where(b < first + EARLY, b - EARLY, b)))
        attend(i // segs, lax.rem(i, segs))

    for c in range(heads):
        @pl.when(meet_at(c) >= blocks)
        def _():
            meet(c)
    for c in range(last - 1):
        @pl.when(finish_at(c) >= blocks)
        def _():
            finish(c)

    weight_copy.wait()

    def product(source, j, part):
        slot = source * heads + 2 * j
        return jnp.dot(
            jnp.concatenate([ctx[slot, part], ctx[slot + 1, part]], axis=1),
            w_ref[pl.ds(pl.multiple_of(slot * DH, 2 * DH), 2 * DH), :],
            preferred_element_type=F32,
        )

    def pair_of(source, j):
        return ctx.at[pl.ds(source * heads + 2 * j, 2)]

    for j in range(pairs - 1):
        for s in range(segs):
            part = rows_of(s)
            sums = product(me_h, j, part)
            acc[part, :] = sums if j == 0 else acc[part, :] + sums

    finish(last - 1)
    finish(last)

    for j in range(pairs - 1):
        for d in range(len(far)):
            for h in (2 * j, 2 * j + 1):
                whole = ctx.at[far[d] * heads + h]
                from_far(d, whole, h).wait_recv()
                relay(d, whole, j).start()

    def cross(d):
        early_done(d, 0, prior_at, early_recv).wait_recv()
        early_done(d, prior_at, SENT, late_recv).wait_recv()
        for s in range(EARLY):
            mem = far_early[d, pl.ds(prior_at, SENT)].astype(F32)[:MEM]
            if s > 0:
                mem = mem + far_early[d, pl.ds(inner_at + (s - 1) * SENT, SENT)].astype(F32)[:MEM]
            value = recall_of(far_early[d, pl.ds(q_at + s * SEG, SEG)], mem)
            value = value + far_early[d, pl.ds(local_at + s * SEG, SEG)].astype(F32)
            ctx[far[d] * heads + last, pl.ds(s * SEG, SEG)] = value.astype(BF16)

    def take(s):
        for d in range(len(far)):
            two = both_of(far[d], s)
            if s < EARLY:
                @pl.when(ahead)
                def _():
                    one = ctx.at[far[d] * heads + last - 1, rows_of(s)]
                    from_far(d, one, last - 1 + s).wait_recv()

                @pl.when(jnp.logical_not(ahead))
                def _():
                    from_far(d, two, last - 1 + s).wait_recv()
            else:
                from_far(d, two, last - 1 + s).wait_recv()
            relay(d, two, pairs - 1 + s).start()

    def twins(s):
        for d in range(len(far)):
            relay(d, both_of(twin[d], s), pairs - 1 + s).wait_recv()

    def tail(sources, s):
        sums = acc[rows_of(s), :]
        for source in sources:
            sums = sums + product(source, pairs - 1, rows_of(s))
        return sums

    def fill(s):
        part = rows_of(s)
        sums = product(me_h, pairs - 1, part) + product(pair_h, pairs - 1, part)
        for j in range(pairs - 1):
            sums = sums + product(pair_h, j, part)
            for d in range(len(far)):
                sums = sums + product(far[d], j, part) + product(twin[d], j, part)
        acc[part, :] = acc[part, :] + sums if pairs > 1 else sums

    for j in range(pairs):
        to_pair(pair_of(pair_h, j), j).wait_recv()
    for j in range(pairs - 1):
        for d in range(len(far)):
            relay(d, pair_of(twin[d], j), j).wait_recv()
    for s in range(segs):
        if s == min(1, segs - 1):
            @pl.when(ahead)
            def _():
                for d in range(len(far)):
                    cross(d)
        if 0 < s <= EARLY:
            take(s - 1)
        fill(s)
    for s in range(EARLY):
        twins(s)
        out_ref[rows_of(s), :] = tail(far + twin, s).astype(BF16)
    for s in range(EARLY, segs - 1):
        take(s)
        twins(s)
        out_ref[rows_of(s), :] = tail(far + twin, s).astype(BF16)
    take(segs - 1)
    acc[rows_of(segs - 1), :] = tail(far, segs - 1)

    pltpu.make_async_remote_copy(
        src_ref=mine, dst_ref=mine, send_sem=x_send, recv_sem=x_recv.at[0],
        device_id=(pair_s, me_h), device_id_type=MESH,
    ).wait_send()

    @pl.loop(z + 1, zs)
    def _(t):
        pltpu.make_async_remote_copy(
            src_ref=plane, dst_ref=plane, send_sem=z_send.at[t - z - 1], recv_sem=z_recv.at[0, 0],
            device_id=(t * 2 + odd, me_h), device_id_type=MESH,
        ).wait_send()

    to_pair(ctx.at[pl.ds(me_h * heads, heads)], 0).wait_send()
    for d in range(len(far)):
        for h in range(last - 1):
            to_far(d, ctx.at[me_h * heads + h], h).wait_send()
        for s in range(EARLY, segs):
            to_far(d, both_of(me_h, s), last - 1 + s).wait_send()

        @pl.when(ahead)
        def _():
            for s in range(EARLY):
                one = ctx.at[me_h * heads + last - 1, rows_of(s)]
                to_far(d, one, last - 1 + s).wait_send()
            early_done(d, 0, prior_at + SENT, early_recv).wait_send()

        @pl.when(jnp.logical_not(ahead))
        def _():
            for s in range(EARLY):
                to_far(d, both_of(me_h, s), last - 1 + s).wait_send()

    twins(segs - 1)
    out_ref[rows_of(segs - 1), :] = tail(twin, segs - 1).astype(BF16)
    for d in range(len(far)):
        relay(d, ctx.at[pl.ds(far[d] * heads, heads)], 0).wait_send()


def body(ns, nh, queries, keys, values, gate_bias, out_weight):
    rows, cols = queries.shape
    depth, outs = out_weight.shape
    segs, heads = rows // SEG, cols // DH
    pairs = heads // 2
    zs = ns // 2
    fars = nh // 2 - 1
    hbm = pl.BlockSpec(memory_space=pl.ANY)
    dma = pltpu.SemaphoreType.DMA
    mem = pltpu.VMEM((heads, MEM, DH), F32)
    sent = pltpu.VMEM((heads, SENT, DH), BF16)
    return pl.pallas_call(
        functools.partial(kernel, ns, nh),
        out_shape=pltpu.VMEM((rows, outs), BF16),
        in_specs=[hbm, hbm, hbm, hbm, hbm],
        out_specs=pl.BlockSpec(memory_space=pltpu.VMEM),
        scratch_shapes=[
            pltpu.VMEM((rows, cols), BF16),
            pltpu.VMEM((heads, 2, rows, DH), BF16),
            pltpu.SMEM((heads,), F32),
            pltpu.VMEM((depth, outs), BF16),
            pltpu.VMEM((heads, rows, DH), F32),
            pltpu.VMEM((heads, segs, MEM, DH), F32),
            mem, sent, sent, sent,
            pltpu.VMEM((zs - 1, heads, SENT, DH), BF16),
            mem,
            pltpu.VMEM((nh * heads, rows, DH), BF16),
            pltpu.VMEM((rows, outs), F32),
            pltpu.VMEM((EARLY * SEG, DH), BF16),
            pltpu.VMEM(((EARLY - 1) * SENT, DH), BF16),
            pltpu.VMEM((SENT, DH), BF16),
            pltpu.VMEM((fars, 2 * EARLY * SEG + EARLY * SENT, DH), BF16),
            dma((heads,)), dma, dma, dma, pltpu.SemaphoreType.REGULAR,
            dma, dma((heads,)), dma((zs - 1,)), dma((zs - 1, heads)),
            dma, dma((pairs,)), dma((fars, heads - 2 + segs)), dma((fars, heads - 2 + segs)),
            dma((fars,)), dma((fars, pairs - 1 + segs)),
            dma((fars,)), dma((fars,)), dma((fars,)),
        ],
        compiler_params=pltpu.CompilerParams(
            collective_id=0, has_side_effects=True, vmem_limit_bytes=56 * 1024 * 1024
        ),
        name="infini_layer",
    )(queries, keys, values, gate_bias, out_weight)


def solution(mesh):
    sizes = dict(mesh.shape)
    return jax.shard_map(
        functools.partial(body, sizes["seq"], sizes["head"]),
        mesh=mesh,
        in_specs=(P("seq", "head"), P("seq", "head"), P("seq", "head"), P("head"), P(None, "head")),
        out_specs=P("seq", "head"),
        check_vma=False,
    )
```
